32 devices in a mesh: tensor: 4 (over x, core), dp: 8 (over z, y).
Axes of the slice: x: 2, y: 2, z: 4, core: 2. Of those that a mesh axis runs over, the one named last changes fastest.
Arguments:
- grads: bfloat16 [8, 4, 8192, 1024], P('dp', None, None, 'tensor'), may hold values from -6 to 6
- param: float32 [4, 8192, 1024], P(None, 'dp', 'tensor'), may hold values from -3 to 3
- q_m: bfloat16 [4, 8192, 1024], P(None, 'dp', 'tensor'), may hold values from -1 to 1
- m_scale: float32 [4], replicated, may hold values from 0.02 to 0.2
- q_v: bfloat16 [4, 8192, 1024], P(None, 'dp', 'tensor'), may hold values from 0.0009994507 to 1
- v_max: float32 [4, 8], P(None, 'tensor'), may hold values from 0.005 to 0.05
- v_exp: float32 [4, 8], P(None, 'tensor'), may hold values from 1 to 10
Outputs:
- new_param: float32 [4, 8192, 1024], P(None, 'dp', 'tensor')
- new_q_m: bfloat16 [4, 8192, 1024], P(None, 'dp', 'tensor')
- new_m_scale: float32 [4], replicated
- new_q_v: bfloat16 [4, 8192, 1024], P(None, 'dp', 'tensor')
- new_v_max: float32 [4, 8], P(None, 'tensor')
- new_v_exp: float32 [4, 8], P(None, 'tensor')
The draws below stay inside these ranges and needn't reach their ends.
All inputs are finite; a program needn't handle non-finite values. Where the reference program divides by a largest or mean magnitude, that divisor is 1e-20 or more.
Results may differ from the reference program's by a relative error of at most 0.001.
Values sent between devices are 32-bit elements; how exact they have to be, the bound alone decides.
A program may use at most 192 MiB of HBM per device.

```python
import math
import jax
import jax.numpy as jnp
from jax import lax

D = 8192
KVW = 1024
HEAD = 128
TENSORS = 4
GROUPS = 8
REPLICAS = 8


def with_spikes(result, rng, source, target, parts, factor):
    def block_of(position):
        return (jnp.arange(result.shape[position]) // (result.shape[position] // parts)).reshape((-1,) + (1,) * (result.ndim - 1 - position))

    one_side = jax.random.permutation(rng, parts)[block_of(target)]
    second = (block_of(target) + parts // 2) % parts
    return jnp.where((block_of(source) == one_side) | (block_of(source) == second), factor * result, result)


def shard_levels(stream_key, dims, split, smallest, largest):
    loudness, own = 1.0, jax.random.fold_in(stream_key, 6)
    for axis_at, shards_of in split:
        steps = jnp.exp(jax.random.uniform(jax.random.fold_in(own, axis_at), (shards_of,), jnp.float32, smallest / len(split), largest / len(split)))
        loudness = loudness * jnp.repeat(steps, dims[axis_at] // shards_of).reshape([-1 if axis == axis_at else 1 for axis in range(len(dims))])
    return loudness


def gaussian(rng, shape, deviation, most, pieces=(), kind=jnp.bfloat16):
    values = jax.random.normal(rng, shape, jnp.float32) * deviation
    if len(pieces) > 0:
        values = shard_levels(rng, shape, pieces, -0.22, 0.18) * values
    return jnp.clip(values, min=-most, max=most).astype(kind)


def heavy_noise(stream_key, shape, scale, most, split, heavy, dtype=jnp.bfloat16):
    values = scale * jax.random.normal(stream_key, shape, jnp.float32)
    if split:
        values = values * shard_levels(stream_key, shape, split, -0.22, 0.18)
    return jnp.clip(with_spikes(values, jax.random.fold_in(stream_key, 3), *heavy), -most, most).astype(dtype)


def setup_inputs(seed: int = 0) -> dict:
    streams_of = jax.random.split(jax.random.key(seed), 8)
    return {
        "grads": heavy_noise(streams_of[0], (REPLICAS, TENSORS, D, KVW), 1.0, 6.0, ((0, 8), (3, 4)), (0, 2, 8, 2.0)),
        "param": gaussian(streams_of[1], (TENSORS, D, KVW), 0.5, 3.0, ((1, 8), (2, 4)), jnp.float32),
        "q_m": jnp.clip(jax.random.uniform(streams_of[2], (TENSORS, D, KVW), jnp.float32, -1.0, 1.0) * shard_levels(streams_of[2], (TENSORS, D, KVW), ((1, 8), (2, 4)), -0.4, 0.0), -1.0, 1.0).astype(jnp.bfloat16),
        "m_scale": jnp.clip(jnp.exp(jax.random.uniform(streams_of[3], (TENSORS,), jnp.float32, math.log(0.02), math.log(0.2))), 0.02, 0.2),
        "q_v": jnp.clip(jnp.exp(math.log(1.0) - 6.9083047 * jax.random.uniform(streams_of[4], (TENSORS, D, KVW), jnp.float32) ** shard_levels(streams_of[4], (TENSORS, D, KVW), ((1, 8), (2, 4)), -0.2, 0.2)), 0.0009994507, 1.0).astype(jnp.bfloat16),
        "v_max": jnp.clip(jnp.exp(math.log(0.05) - 2.3025851 * jax.random.uniform(streams_of[5], (TENSORS, GROUPS), jnp.float32) ** shard_levels(streams_of[5], (TENSORS, GROUPS), ((1, 4),), -0.2, 0.2)), 0.005, 0.05),
        "v_exp": jnp.clip(1.0 + 9.0 * jax.random.uniform(streams_of[6], (TENSORS, GROUPS), jnp.float32) ** shard_levels(streams_of[6], (TENSORS, GROUPS), ((1, 4),), -0.2, 0.2), 1.0, 10.0),
    }


def reference(grads, param, q_m, m_scale, q_v, v_max, v_exp):

    def add_one(index, total):
        return total + lax.dynamic_index_in_dim(grads, index, 0, keepdims=False).astype(jnp.float32)
    summed = lax.fori_loop(0, REPLICAS, add_one, jnp.zeros((TENSORS, D, KVW), jnp.float32))
    grad = (summed / REPLICAS).reshape(TENSORS, D, GROUPS, HEAD)
    m_old = m_scale[:, None, None, None] * q_m.astype(jnp.float32).reshape(TENSORS, D, GROUPS, HEAD)
    stored = q_v.astype(jnp.float32).reshape(TENSORS, D, GROUPS, HEAD)
    v_old = v_max[:, None, :, None] * jnp.exp(jnp.log(stored) / v_exp[:, None, :, None])
    m_new = 0.9 * m_old + 0.1 * grad
    v_new = 0.95 * v_old + 0.05 * grad * grad
    weights = param.reshape(TENSORS, D, GROUPS, HEAD)
    new_param = weights - 0.02 * (m_new / (jnp.sqrt(v_new) + 1e-08) + 0.1 * weights)
    new_m_scale = lax.optimization_barrier(jnp.max(jnp.abs(m_new), axis=(1, 2, 3))) + 1e-06
    new_v_max = lax.optimization_barrier(jnp.max(v_new, axis=(1, 3)))
    v_low = lax.optimization_barrier(jnp.min(v_new, axis=(1, 3)))
    new_v_exp = 12.343 / jnp.maximum(jnp.log(new_v_max / v_low), 1.0)
    new_q_m = (m_new / new_m_scale[:, None, None, None]).astype(jnp.bfloat16)
    new_q_v = jnp.exp(new_v_exp[:, None, :, None] * jnp.log(v_new / new_v_max[:, None, :, None])).astype(jnp.bfloat16)
    shape = (TENSORS, D, KVW)
    return (new_param.reshape(shape), new_q_m.reshape(shape), new_m_scale, new_q_v.reshape(shape), new_v_max, new_v_exp)
```

```python
import functools

import jax
import jax.numpy as jnp
from jax import lax
from jax.experimental import pallas as pl
from jax.experimental.pallas import tpu as pltpu
from jax.sharding import PartitionSpec as P

MESH = pl.DeviceIdType.MESH
STEP = 32
Z_FIRST = 5 / 9


def kernel(n, peers, rows_a, rows_b, *refs):
    (grads, param, q_m, q_v, m_scale, v_max, v_exp,
     out_p, out_m, out_v, out_s,
     raw, a_cast, a_ring, a_side, b_cast, b_side, b_ring,
     par, qm, qv, m_new, v_new, stat, stat_in, peak, peak_in,
     raw_sem, in_sem, out_sem,
     a_send, a_recv, as_send, as_recv, bs_send, bs_recv, b_send, b_recv,
     st_send, st_recv, pk_send, pk_recv) = refs
    count, _, rows, width = grads.shape
    groups = v_max.shape[1]
    lanes = width // groups
    nz = n // 2
    me = lax.axis_index("dp")
    mt = lax.axis_index("tensor")
    y = lax.rem(me, 2)
    z = me // 2
    other = z * 2 + (1 - y)
    signs = (1, -1)
    a_off = (0, rows_a)
    b_off = (2 * rows_a, 2 * rows_a + rows_b)

    def at_z(offset):
        return lax.rem(z + (offset % nz), nz)

    def ring_to(s):
        return at_z(s) * 2 + y

    barrier = pltpu.get_barrier_semaphore()

    raws = [pltpu.make_async_copy(grads.at[t], raw.at[t % 3], raw_sem.at[t]) for t in range(count)]
    ins = [[pltpu.make_async_copy(src.at[t], dst.at[t], in_sem.at[t, i])
            for i, (src, dst) in enumerate(((q_m, qm), (q_v, qv), (param, par)))] for t in range(count)]
    for t in range(min(3, count)):
        raws[t].start()
    for t in range(count):
        for c in ins[t]:
            c.start()

    def greet(o, _):
        pl.semaphore_signal(barrier, inc=1, device_id={"dp": lax.rem(me + o, n)}, device_id_type=MESH)
        return 0
    lax.fori_loop(1, n, greet, 0)

    def greet_t(o, _):
        pl.semaphore_signal(barrier, inc=1, device_id={"tensor": lax.rem(mt + o, peers)}, device_id_type=MESH)
        return 0
    lax.fori_loop(1, peers, greet_t, 0)
    pl.semaphore_wait(barrier, n - 1 + peers - 1)

    unsent = {}

    def send(key, src, dst, s_sem, r_sem, to):
        c = pltpu.make_async_remote_copy(src_ref=src, dst_ref=dst, send_sem=s_sem, recv_sem=r_sem,
                                         device_id={"dp": to}, device_id_type=MESH)
        c.start()
        unsent[key] = c
        return c

    def sent(key):
        unsent.pop(key).wait_send()

    def loop(total, body):
        def one(i, _):
            body(pl.multiple_of(i * STEP, STEP))
            return 0
        lax.fori_loop(0, total // STEP, one, 0)

    def mine(t, k, side, at, i):
        return raw[t % 3, k * 2 + side, pl.ds(pl.multiple_of(at + i, STEP), STEP), :].astype(jnp.float32)

    live = {}

    def cast(t):
        raws[t].wait()
        for d, s in enumerate(signs):
            if t >= 2:
                sent(("a", t - 2, d, 0))
            k = at_z(-s)
            for side in range(2):
                def body(i):
                    a_cast[t % 2, d, side, pl.ds(i, STEP), :] = mine(t, k, side, a_off[d], i)
                loop(rows_a, body)
            live["a", t, d, 0] = send(("a", t, d, 0), a_cast.at[t % 2, d], a_ring.at[t, d, 0],
                                      a_send.at[t, d, 0], a_recv.at[t, d, 0], ring_to(s))
        for d, s in enumerate(signs):
            if t >= 2:
                sent(("bs", t - 2, d))

            def block(k, _):
                def body(i):
                    b_cast[t % 2, d, k, pl.ds(i, STEP), :] = mine(t, k, 1 - y, b_off[d], i)
                loop(rows_b, body)
                return 0
            lax.fori_loop(0, nz, block, 0)
            live["bs", t, d] = send(("bs", t, d), b_cast.at[t % 2, d], b_side.at[t, d],
                                    bs_send.at[t, d], bs_recv.at[t, d], other)

    def a_step(t, j):
        for d, s in enumerate(signs):
            live["a", t, d, j].wait_recv()
            k = at_z(-s * (j + 2))
            for side in range(2):
                def body(i):
                    at = (t, d, j, side, pl.ds(i, STEP), slice(None))
                    a_ring[at] = a_ring[at] + mine(t, k, side, a_off[d], i)
                loop(rows_a, body)
            if j < nz - 2:
                live["a", t, d, j + 1] = send(("a", t, d, j + 1), a_ring.at[t, d, j], a_ring.at[t, d, j + 1],
                                              a_send.at[t, d, j + 1], a_recv.at[t, d, j + 1], ring_to(s))
            else:
                live["as", t, d] = send(("as", t, d), a_ring.at[t, d, j, 1 - y], a_side.at[t, d],
                                        as_send.at[t, d], as_recv.at[t, d], other)

    def b_start(t):
        for d, s in enumerate(signs):
            live["bs", t, d].wait_recv()
            k = at_z(-s)

            def body(i):
                at = (t, d, k, pl.ds(i, STEP), slice(None))
                b_side[at] = b_side[at] + mine(t, k, y, b_off[d], i)
            loop(rows_b, body)
            live["b", t, d, 0] = send(("b", t, d, 0), b_side.at[t, d, k], b_ring.at[t, d, 0],
                                      b_send.at[t, d, 0], b_recv.at[t, d, 0], ring_to(s))

    def b_step(t, j):
        for d, s in enumerate(signs):
            live["b", t, d, j].wait_recv()
            if j == nz - 2:
                def total(i):
                    rows_i = pl.ds(i, STEP)
                    return b_ring[t, d, j, rows_i, :] + (b_side[t, d, z, rows_i, :] + mine(t, z, y, b_off[d], i))
                update(t, b_off[d], rows_b, total)
                continue
            k = at_z(-s * (j + 2))

            def body(i):
                at = (t, d, j, pl.ds(i, STEP), slice(None))
                b_ring[at] = b_ring[at] + (b_side[t, d, k, pl.ds(i, STEP), :] + mine(t, k, y, b_off[d], i))
            loop(rows_b, body)
            live["b", t, d, j + 1] = send(("b", t, d, j + 1), b_ring.at[t, d, j], b_ring.at[t, d, j + 1],
                                          b_send.at[t, d, j + 1], b_recv.at[t, d, j + 1], ring_to(s))

    def a_last(t):
        for c in ins[t]:
            c.wait()
        stat[t] = jnp.full(stat.shape[1:], -jnp.inf, jnp.float32)
        for d in range(2):
            live["as", t, d].wait_recv()

            def total(i):
                rows_i = pl.ds(i, STEP)
                return a_ring[t, d, nz - 2, y, rows_i, :] + a_side[t, d, rows_i, :]
            update(t, a_off[d], rows_a, total)

    def update(t, base, length, total):
        scale = m_scale[t]

        def fold(x):
            return jnp.max(x.reshape(STEP // 8, 8, lanes), axis=0)

        def one(it, carry):
            i = pl.multiple_of(it * STEP, STEP)
            whole = total(i) * (1.0 / n)
            rows_i = pl.ds(pl.multiple_of(base + i, STEP), STEP)
            top_m, tops, lows = carry
            new_tops, new_lows = [], []
            for g in range(groups):
                cols = slice(g * lanes, (g + 1) * lanes)
                grad = whole[:, cols]
                m_old = scale * qm[t, rows_i, cols].astype(jnp.float32)
                stored = qv[t, rows_i, cols].astype(jnp.float32)
                inv = 1.0 / jnp.full((1, lanes), v_exp[t, g], jnp.float32)
                v_old = v_max[t, g] * jnp.exp(jnp.log(stored) * inv)
                m = 0.9 * m_old + 0.1 * grad
                v = 0.95 * v_old + 0.05 * grad * grad
                w = par[t, rows_i, cols]
                par[t, rows_i, cols] = w - 0.02 * (m / (jnp.sqrt(v) + 1e-08) + 0.1 * w)
                m_new[t % 2, rows_i, cols] = m
                v_new[t % 2, rows_i, cols] = v
                top_m = jnp.maximum(top_m, fold(jnp.abs(m)))
                new_tops.append(jnp.maximum(tops[g], fold(v)))
                new_lows.append(jnp.maximum(lows[g], fold(-v)))
            return top_m, tuple(new_tops), tuple(new_lows)
        least = jnp.full((8, lanes), -jnp.inf, jnp.float32)
        top_m, tops, lows = lax.fori_loop(0, length // STEP, one, (least, (least,) * groups, (least,) * groups))
        for row, value in enumerate((top_m,) + tops + lows):
            stat[t, row:row + 1, :] = jnp.maximum(stat[t, row:row + 1, :], jnp.max(value, axis=0, keepdims=True))

    def stat_copy(t, o):
        return pltpu.make_async_remote_copy(
            src_ref=stat.at[t], dst_ref=stat_in.at[t, o], send_sem=st_send.at[t, o], recv_sem=st_recv.at[t, o],
            device_id={"dp": lax.rem(me + o, n)}, device_id_type=MESH)

    def peak_copy(t, o):
        return pltpu.make_async_remote_copy(
            src_ref=peak.at[t], dst_ref=peak_in.at[t, o], send_sem=pk_send.at[t, o], recv_sem=pk_recv.at[t, o],
            device_id={"tensor": lax.rem(mt + o, peers)}, device_id_type=MESH)

    def each(lo, hi, act):
        def one(o, _):
            act(o)
            return 0
        lax.fori_loop(lo, hi, one, 0)

    outs = []

    def give(src, dst, t, i):
        c = pltpu.make_async_copy(src.at[t], dst.at[t], out_sem.at[t, i])
        c.start()
        outs.append(c)

    def share(t):
        give(par, out_p, t, 0)
        each(1, n, lambda o: stat_copy(t, o).start())

    def finish(t):
        each(1, n, lambda o: stat_copy(t, o).wait_recv())
        best = lax.fori_loop(1, n, lambda o, b: jnp.maximum(b, stat_in[t, o]), stat[t])
        best = jnp.broadcast_to(jnp.max(best, axis=1, keepdims=True), best.shape)
        peak[t] = best
        each(1, peers, lambda o: peak_copy(t, o).start())
        exps, invs = [], []
        for g in range(groups):
            top = best[1 + g:2 + g, :]
            low = -best[1 + groups + g:2 + groups + g, :]
            exps.append(12.343 / jnp.maximum(jnp.log(top / low), 1.0))
            invs.append(1.0 / top)
            out_s[t, 1 + g:2 + g, :] = top
            out_s[t, 1 + groups + g:2 + groups + g, :] = exps[g]

        def body(i):
            for g in range(groups):
                at = (pl.ds(i, STEP), slice(g * lanes, (g + 1) * lanes))
                value = jnp.exp(exps[g] * jnp.log(v_new[(t % 2,) + at] * invs[g]))
                qv[(t,) + at] = value.astype(jnp.bfloat16)
        loop(rows, body)
        give(qv, out_v, t, 1)
        each(1, peers, lambda o: peak_copy(t, o).wait_recv())
        whole = lax.fori_loop(1, peers, lambda o, b: jnp.maximum(b, peak_in[t, o]), best)[0:1, :] + 1e-06
        out_s[t, 0:1, :] = whole
        inverse = 1.0 / whole

        def body_m(i):
            for g in range(groups):
                at = (pl.ds(i, STEP), slice(g * lanes, (g + 1) * lanes))
                qm[(t,) + at] = (m_new[(t % 2,) + at] * inverse).astype(jnp.bfloat16)
        loop(rows, body_m)
        give(qm, out_m, t, 2)

    cast(0)
    for p in range(count + 1):
        if p + 1 < count:
            cast(p + 1)
        if p >= 1:
            b_start(p - 1)
        for j in range(nz - 1):
            if p < count:
                a_step(p, j)
            if p >= 1 and j == nz - 2:
                a_last(p - 1)
            if p >= 1:
                b_step(p - 1, j)
        if p >= 1:
            if p + 2 < count:
                raws[p + 2].start()
            share(p - 1)
        if p >= 2:
            finish(p - 2)
    finish(count - 1)

    for key in list(unsent):
        sent(key)
    for t in range(count):
        each(1, n, lambda o: stat_copy(t, o).wait_send())
        each(1, peers, lambda o: peak_copy(t, o).wait_send())
    for c in outs:
        c.wait()


def on_device(n, peers, grads, param, q_m, m_scale, q_v, v_max, v_exp):
    count, rows, width = q_m.shape
    groups = v_max.shape[1]
    lanes = width // groups
    nz = n // 2
    rows_a = min(max(STEP, round(rows * Z_FIRST / 2 / STEP) * STEP), rows // 2 - STEP)
    rows_b = rows // 2 - rows_a
    kinds = -(-(1 + 2 * groups) // 8) * 8
    f32, bf16 = jnp.float32, jnp.bfloat16
    dma = pltpu.SemaphoreType.DMA
    hbm = pl.BlockSpec(memory_space=pl.ANY)
    smem = pl.BlockSpec(memory_space=pltpu.SMEM)
    new_param, new_q_m, new_q_v, stats = pl.pallas_call(
        functools.partial(kernel, n, peers, rows_a, rows_b),
        out_shape=(
            jax.ShapeDtypeStruct(param.shape, f32),
            jax.ShapeDtypeStruct(q_m.shape, bf16),
            jax.ShapeDtypeStruct(q_v.shape, bf16),
            jax.ShapeDtypeStruct((count, kinds, lanes), f32),
        ),
        in_specs=[hbm] * 4 + [smem] * 3,
        out_specs=(hbm, hbm, hbm, pl.BlockSpec(memory_space=pltpu.VMEM)),
        scratch_shapes=[
            pltpu.VMEM((3, n, rows, width), bf16),
            pltpu.VMEM((2, 2, 2, rows_a, width), f32),
            pltpu.VMEM((count, 2, nz - 1, 2, rows_a, width), f32),
            pltpu.VMEM((count, 2, rows_a, width), f32),
            pltpu.VMEM((2, 2, nz, rows_b, width), f32),
            pltpu.VMEM((count, 2, nz, rows_b, width), f32),
            pltpu.VMEM((count, 2, nz - 1, rows_b, width), f32),
            pltpu.VMEM(param.shape, f32),
            pltpu.VMEM(q_m.shape, bf16),
            pltpu.VMEM(q_v.shape, bf16),
            pltpu.VMEM((2, rows, width), f32),
            pltpu.VMEM((2, rows, width), f32),
            pltpu.VMEM((count, kinds, lanes), f32),
            pltpu.VMEM((count, n, kinds, lanes), f32),
            pltpu.VMEM((count, kinds, lanes), f32),
            pltpu.VMEM((count, peers, kinds, lanes), f32),
            dma((count,)), dma((count, 3)), dma((count, 3)),
            dma((count, 2, nz - 1)), dma((count, 2, nz - 1)),
            dma((count, 2)), dma((count, 2)),
            dma((count, 2)), dma((count, 2)),
            dma((count, 2, nz - 1)), dma((count, 2, nz - 1)),
            dma((count, n)), dma((count, n)),
            dma((count, peers)), dma((count, peers)),
        ],
        compiler_params=pltpu.CompilerParams(
            collective_id=0, has_side_effects=True, vmem_limit_bytes=67043328
        ),
    )(grads[0].reshape(count, n, rows, width), param, q_m, q_v, m_scale, v_max, v_exp)
    new_m_scale = stats[:, 0, 0]
    group_top = stats[:, 1:1 + groups, 0]
    new_v_exp = stats[:, 1 + groups:1 + 2 * groups, 0]
    return new_param, new_q_m, new_m_scale, new_q_v, group_top, new_v_exp


def solution(mesh):
    in_specs = (
        P("dp", None, None, "tensor"),
        P(None, "dp", "tensor"),
        P(None, "dp", "tensor"),
        P(),
        P(None, "dp", "tensor"),
        P(None, "tensor"),
        P(None, "tensor"),
    )
    out_specs = (
        P(None, "dp", "tensor"),
        P(None, "dp", "tensor"),
        P(),
        P(None, "dp", "tensor"),
        P(None, "tensor"),
        P(None, "tensor"),
    )
    return jax.shard_map(
        functools.partial(on_device, mesh.shape["dp"], mesh.shape["tensor"]),
        mesh=mesh, in_specs=in_specs, out_specs=out_specs, check_vma=False
    )
```

```python
import functools

import jax
import jax.numpy as jnp
from jax import lax
from jax.experimental import pallas as pl
from jax.experimental.pallas import tpu as pltpu
from jax.sharding import PartitionSpec as P

MESH = pl.DeviceIdType.MESH
STEP = 32
Z_FIRST = 0.25


def kernel(n, peers, rows_a, rows_b, *refs):
    (grads, param, q_m, q_v, m_scale, v_max, v_exp,
     out_p, out_m, out_v, out_s,
     raw, a_cast, a_ring, a_side, b_cast, b_side, b_ring,
     par, qm, qv, m_new, v_new, stat, stat_in, peak, peak_in,
     raw_sem, in_sem, out_sem,
     a_send, a_recv, as_send, as_recv, bs_send, bs_recv, b_send, b_recv,
     st_send, st_recv, pk_send, pk_recv) = refs
    count, _, rows, width = grads.shape
    groups = v_max.shape[1]
    lanes = width // groups
    nz = n // 2
    me = lax.axis_index("dp")
    mt = lax.axis_index("tensor")
    y = lax.rem(me, 2)
    z = me // 2
    other = z * 2 + (1 - y)
    signs = (1, -1)
    a_off = (0, rows_a)
    b_off = (2 * rows_a, 2 * rows_a + rows_b)

    def at_z(offset):
        return lax.rem(z + (offset % nz), nz)

    def ring_to(s):
        return at_z(s) * 2 + y

    barrier = pltpu.get_barrier_semaphore()

    raws = [pltpu.make_async_copy(grads.at[t], raw.at[t % 3], raw_sem.at[t]) for t in range(count)]
    ins = [[pltpu.make_async_copy(src.at[t], dst.at[t], in_sem.at[t, i])
            for i, (src, dst) in enumerate(((q_m, qm), (q_v, qv), (param, par)))] for t in range(count)]
    for t in range(min(3, count)):
        raws[t].start()
    for t in range(count):
        for c in ins[t]:
            c.start()

    def greet(o, _):
        pl.semaphore_signal(barrier, inc=1, device_id={"dp": lax.rem(me + o, n)}, device_id_type=MESH)
        return 0
    lax.fori_loop(1, n, greet, 0)

    def greet_t(o, _):
        pl.semaphore_signal(barrier, inc=1, device_id={"tensor": lax.rem(mt + o, peers)}, device_id_type=MESH)
        return 0
    lax.fori_loop(1, peers, greet_t, 0)
    pl.semaphore_wait(barrier, n - 1 + peers - 1)

    unsent = {}

    def send(key, src, dst, s_sem, r_sem, to):
        c = pltpu.make_async_remote_copy(src_ref=src, dst_ref=dst, send_sem=s_sem, recv_sem=r_sem,
                                         device_id={"dp": to}, device_id_type=MESH)
        c.start()
        unsent[key] = c
        return c

    def sent(key):
        unsent.pop(key).wait_send()

    def loop(total, body):
        def one(i, _):
            body(pl.multiple_of(i * STEP, STEP))
            return 0
        lax.fori_loop(0, total // STEP, one, 0)

    def mine(t, k, side, at, i):
        return raw[t % 3, k * 2 + side, pl.ds(pl.multiple_of(at + i, STEP), STEP), :].astype(jnp.float32)

    live = {}

    def cast(t):
        raws[t].wait()
        for d, s in enumerate(signs):
            if t >= 2:
                sent(("a", t - 2, d, 0))
            k = at_z(-s)
            for side in range(2):
                def body(i):
                    a_cast[t % 2, d, side, pl.ds(i, STEP), :] = mine(t, k, side, a_off[d], i)
                loop(rows_a, body)
            live["a", t, d, 0] = send(("a", t, d, 0), a_cast.at[t % 2, d], a_ring.at[t, d, 0],
                                      a_send.at[t, d, 0], a_recv.at[t, d, 0], ring_to(s))
        for d, s in enumerate(signs):
            if t >= 2:
                sent(("bs", t - 2, d))

            def block(k, _):
                def body(i):
                    b_cast[t % 2, d, k, pl.ds(i, STEP), :] = mine(t, k, 1 - y, b_off[d], i)
                loop(rows_b, body)
                return 0
            lax.fori_loop(0, nz, block, 0)
            live["bs", t, d] = send(("bs", t, d), b_cast.at[t % 2, d], b_side.at[t, d],
                                    bs_send.at[t, d], bs_recv.at[t, d], other)

    def a_step(t, j):
        for d, s in enumerate(signs):
            live["a", t, d, j].wait_recv()
            k = at_z(-s * (j + 2))
            for side in range(2):
                def body(i):
                    at = (t, d, j, side, pl.ds(i, STEP), slice(None))
                    a_ring[at] = a_ring[at] + mine(t, k, side, a_off[d], i)
                loop(rows_a, body)
            if j < nz - 2:
                live["a", t, d, j + 1] = send(("a", t, d, j + 1), a_ring.at[t, d, j], a_ring.at[t, d, j + 1],
                                              a_send.at[t, d, j + 1], a_recv.at[t, d, j + 1], ring_to(s))
            else:
                live["as", t, d] = send(("as", t, d), a_ring.at[t, d, j, 1 - y], a_side.at[t, d],
                                        as_send.at[t, d], as_recv.at[t, d], other)

    def b_start(t):
        for d, s in enumerate(signs):
            live["bs", t, d].wait_recv()
            k = at_z(-s)

            def body(i):
                at = (t, d, k, pl.ds(i, STEP), slice(None))
                b_side[at] = b_side[at] + mine(t, k, y, b_off[d], i)
            loop(rows_b, body)
            live["b", t, d, 0] = send(("b", t, d, 0), b_side.at[t, d, k], b_ring.at[t, d, 0],
                                      b_send.at[t, d, 0], b_recv.at[t, d, 0], ring_to(s))

    def b_step(t, j):
        for d, s in enumerate(signs):
            live["b", t, d, j].wait_recv()
            if j == nz - 2:
                def total(i):
                    rows_i = pl.ds(i, STEP)
                    return b_ring[t, d, j, rows_i, :] + (b_side[t, d, z, rows_i, :] + mine(t, z, y, b_off[d], i))
                update(t, b_off[d], rows_b, total)
                continue
            k = at_z(-s * (j + 2))

            def body(i):
                at = (t, d, j, pl.ds(i, STEP), slice(None))
                b_ring[at] = b_ring[at] + (b_side[t, d, k, pl.ds(i, STEP), :] + mine(t, k, y, b_off[d], i))
            loop(rows_b, body)
            live["b", t, d, j + 1] = send(("b", t, d, j + 1), b_ring.at[t, d, j], b_ring.at[t, d, j + 1],
                                          b_send.at[t, d, j + 1], b_recv.at[t, d, j + 1], ring_to(s))

    def a_last(t):
        for c in ins[t]:
            c.wait()
        stat[t] = jnp.full(stat.shape[1:], -jnp.inf, jnp.float32)
        for d in range(2):
            live["as", t, d].wait_recv()

            def total(i):
                rows_i = pl.ds(i, STEP)
                return a_ring[t, d, nz - 2, y, rows_i, :] + a_side[t, d, rows_i, :]
            update(t, a_off[d], rows_a, total)

    def update(t, base, length, total):
        scale = m_scale[t]

        def fold(x):
            return jnp.max(x.reshape(STEP // 8, 8, lanes), axis=0)

        def one(it, carry):
            i = pl.multiple_of(it * STEP, STEP)
            whole = total(i) * (1.0 / n)
            rows_i = pl.ds(pl.multiple_of(base + i, STEP), STEP)
            top_m, tops, lows = carry
            new_tops, new_lows = [], []
            for g in range(groups):
                cols = slice(g * lanes, (g + 1) * lanes)
                grad = whole[:, cols]
                m_old = scale * qm[t, rows_i, cols].astype(jnp.float32)
                stored = qv[t, rows_i, cols].astype(jnp.float32)
                inv = 1.0 / jnp.full((1, lanes), v_exp[t, g], jnp.float32)
                v_old = v_max[t, g] * jnp.exp(jnp.log(stored) * inv)
                m = 0.9 * m_old + 0.1 * grad
                v = 0.95 * v_old + 0.05 * grad * grad
                w = par[t, rows_i, cols]
                par[t, rows_i, cols] = w - 0.02 * (m / (jnp.sqrt(v) + 1e-08) + 0.1 * w)
                m_new[t % 2, rows_i, cols] = m
                v_new[t % 2, rows_i, cols] = v
                top_m = jnp.maximum(top_m, fold(jnp.abs(m)))
                new_tops.append(jnp.maximum(tops[g], fold(v)))
                new_lows.append(jnp.maximum(lows[g], fold(-v)))
            return top_m, tuple(new_tops), tuple(new_lows)
        least = jnp.full((8, lanes), -jnp.inf, jnp.float32)
        top_m, tops, lows = lax.fori_loop(0, length // STEP, one, (least, (least,) * groups, (least,) * groups))
        for row, value in enumerate((top_m,) + tops + lows):
            stat[t, row:row + 1, :] = jnp.maximum(stat[t, row:row + 1, :], jnp.max(value, axis=0, keepdims=True))

    def stat_copy(t, o):
        return pltpu.make_async_remote_copy(
            src_ref=stat.at[t], dst_ref=stat_in.at[t, o], send_sem=st_send.at[t, o], recv_sem=st_recv.at[t, o],
            device_id={"dp": lax.rem(me + o, n)}, device_id_type=MESH)

    def peak_copy(t, o):
        return pltpu.make_async_remote_copy(
            src_ref=peak.at[t], dst_ref=peak_in.at[t, o], send_sem=pk_send.at[t, o], recv_sem=pk_recv.at[t, o],
            device_id={"tensor": lax.rem(mt + o, peers)}, device_id_type=MESH)

    def each(lo, hi, act):
        def one(o, _):
            act(o)
            return 0
        lax.fori_loop(lo, hi, one, 0)

    outs = []

    def give(src, dst, t, i):
        c = pltpu.make_async_copy(src.at[t], dst.at[t], out_sem.at[t, i])
        c.start()
        outs.append(c)

    def share(t):
        give(par, out_p, t, 0)
        each(1, n, lambda o: stat_copy(t, o).start())

    def finish(t):
        each(1, n, lambda o: stat_copy(t, o).wait_recv())
        best = lax.fori_loop(1, n, lambda o, b: jnp.maximum(b, stat_in[t, o]), stat[t])
        best = jnp.broadcast_to(jnp.max(best, axis=1, keepdims=True), best.shape)
        peak[t] = best
        each(1, peers, lambda o: peak_copy(t, o).start())
        exps, invs = [], []
        for g in range(groups):
            top = best[1 + g:2 + g, :]
            low = -best[1 + groups + g:2 + groups + g, :]
            exps.append(12.343 / jnp.maximum(jnp.log(top / low), 1.0))
            invs.append(1.0 / top)
            out_s[t, 1 + g:2 + g, :] = top
            out_s[t, 1 + groups + g:2 + groups + g, :] = exps[g]

        def body(i):
            for g in range(groups):
                at = (pl.ds(i, STEP), slice(g * lanes, (g + 1) * lanes))
                value = jnp.exp(exps[g] * jnp.log(v_new[(t % 2,) + at] * invs[g]))
                qv[(t,) + at] = value.astype(jnp.bfloat16)
        loop(rows, body)
        give(qv, out_v, t, 1)
        each(1, peers, lambda o: peak_copy(t, o).wait_recv())
        whole = lax.fori_loop(1, peers, lambda o, b: jnp.maximum(b, peak_in[t, o]), best)[0:1, :] + 1e-06
        out_s[t, 0:1, :] = whole
        inverse = 1.0 / whole

        def body_m(i):
            for g in range(groups):
                at = (pl.ds(i, STEP), slice(g * lanes, (g + 1) * lanes))
                qm[(t,) + at] = (m_new[(t % 2,) + at] * inverse).astype(jnp.bfloat16)
        loop(rows, body_m)
        give(qm, out_m, t, 2)

    cast(0)
    for p in range(count + 1):
        if p + 1 < count:
            cast(p + 1)
        if p >= 1:
            b_start(p - 1)
        for j in range(nz - 1):
            if p < count:
                a_step(p, j)
            if p >= 1 and j == nz - 2:
                a_last(p - 1)
            if p >= 1:
                b_step(p - 1, j)
        if p >= 1:
            if p + 2 < count:
                raws[p + 2].start()
            share(p - 1)
        if p >= 2:
            finish(p - 2)
    finish(count - 1)

    for key in list(unsent):
        sent(key)
    for t in range(count):
        each(1, n, lambda o: stat_copy(t, o).wait_send())
        each(1, peers, lambda o: peak_copy(t, o).wait_send())
    for c in outs:
        c.wait()


def on_device(n, peers, grads, param, q_m, m_scale, q_v, v_max, v_exp):
    count, rows, width = q_m.shape
    groups = v_max.shape[1]
    lanes = width // groups
    nz = n // 2
    rows_a = min(max(STEP, round(rows * Z_FIRST / 2 / STEP) * STEP), rows // 2 - STEP)
    rows_b = rows // 2 - rows_a
    kinds = -(-(1 + 2 * groups) // 8) * 8
    f32, bf16 = jnp.float32, jnp.bfloat16
    dma = pltpu.SemaphoreType.DMA
    hbm = pl.BlockSpec(memory_space=pl.ANY)
    smem = pl.BlockSpec(memory_space=pltpu.SMEM)
    new_param, new_q_m, new_q_v, stats = pl.pallas_call(
        functools.partial(kernel, n, peers, rows_a, rows_b),
        out_shape=(
            jax.ShapeDtypeStruct(param.shape, f32),
            jax.ShapeDtypeStruct(q_m.shape, bf16),
            jax.ShapeDtypeStruct(q_v.shape, bf16),
            jax.ShapeDtypeStruct((count, kinds, lanes), f32),
        ),
        in_specs=[hbm] * 4 + [smem] * 3,
        out_specs=(hbm, hbm, hbm, pl.BlockSpec(memory_space=pltpu.VMEM)),
        scratch_shapes=[
            pltpu.VMEM((3, n, rows, width), bf16),
            pltpu.VMEM((2, 2, 2, rows_a, width), f32),
            pltpu.VMEM((count, 2, nz - 1, 2, rows_a, width), f32),
            pltpu.VMEM((count, 2, rows_a, width), f32),
            pltpu.VMEM((2, 2, nz, rows_b, width), f32),
            pltpu.VMEM((count, 2, nz, rows_b, width), f32),
            pltpu.VMEM((count, 2, nz - 1, rows_b, width), f32),
            pltpu.VMEM(param.shape, f32),
            pltpu.VMEM(q_m.shape, bf16),
            pltpu.VMEM(q_v.shape, bf16),
            pltpu.VMEM((2, rows, width), f32),
            pltpu.VMEM((2, rows, width), f32),
            pltpu.VMEM((count, kinds, lanes), f32),
            pltpu.VMEM((count, n, kinds, lanes), f32),
            pltpu.VMEM((count, kinds, lanes), f32),
            pltpu.VMEM((count, peers, kinds, lanes), f32),
            dma((count,)), dma((count, 3)), dma((count, 3)),
            dma((count, 2, nz - 1)), dma((count, 2, nz - 1)),
            dma((count, 2)), dma((count, 2)),
            dma((count, 2)), dma((count, 2)),
            dma((count, 2, nz - 1)), dma((count, 2, nz - 1)),
            dma((count, n)), dma((count, n)),
            dma((count, peers)), dma((count, peers)),
        ],
        compiler_params=pltpu.CompilerParams(
            collective_id=0, has_side_effects=True, vmem_limit_bytes=67043328
        ),
    )(grads[0].reshape(count, n, rows, width), param, q_m, q_v, m_scale, v_max, v_exp)
    new_m_scale = stats[:, 0, 0]
    group_top = stats[:, 1:1 + groups, 0]
    new_v_exp = stats[:, 1 + groups:1 + 2 * groups, 0]
    return new_param, new_q_m, new_m_scale, new_q_v, group_top, new_v_exp


def solution(mesh):
    in_specs = (
        P("dp", None, None, "tensor"),
        P(None, "dp", "tensor"),
        P(None, "dp", "tensor"),
        P(),
        P(None, "dp", "tensor"),
        P(None, "tensor"),
        P(None, "tensor"),
    )
    out_specs = (
        P(None, "dp", "tensor"),
        P(None, "dp", "tensor"),
        P(),
        P(None, "dp", "tensor"),
        P(None, "tensor"),
        P(None, "tensor"),
    )
    return jax.shard_map(
        functools.partial(on_device, mesh.shape["dp"], mesh.shape["tensor"]),
        mesh=mesh, in_specs=in_specs, out_specs=out_specs, check_vma=False
    )
```
